32 devices in a mesh: dp: 8 (over y, x, core), mp: 4 (over z).
Axes of the slice: x: 2, y: 2, z: 4, core: 2. Of those that a mesh axis runs over, the one named last changes fastest.
Arguments:
- tokens: bfloat16 [6144, 6144], P('dp', 'mp'), may hold values from -6 to 6
- ln_gain: bfloat16 [6144], P('mp'), may hold values from 0.5 to 1.5
- weights: bfloat16 [6144, 12288], P('dp', 'mp'), may hold values from -0.078125 to 0.078125
- grad_partials: bfloat16 [8, 6144, 12288], P('dp', None, 'mp'), may hold values from -40 to 40, as said below
Outputs:
- hidden: bfloat16 [6144, 12288], P('dp', 'mp')
- perturbed_weights: bfloat16 [6144, 12288], P('dp', 'mp')
The draws below stay inside these ranges and needn't reach their ends.
Inputs may be any that keep to these rules, and one draw needn't show every extreme that they name: `grad_partials`: each slice along the first dimension is one data shard's gradient.
All inputs are finite; a program needn't handle non-finite values.
Results may differ from the reference program's by a relative error of at most 0.012.
Values may be sent and summed in bfloat16 or wider, within the bound.
A program may use at most 192 MiB of HBM per device.

```python
import math
import jax
import jax.numpy as jnp
from jax import lax

D = 6144
FF = 12288
TOKENS = 6144
N_DP = 8
N_MP = 4


def draw_grad_partials(key, part):
    key_rows, key_cols, key_own = jax.random.split(key, 3)
    row_scale = jnp.exp(jax.random.uniform(key_rows, (1, D, 1), jnp.float32, 0.0, math.log(10.0)))
    col_scale = jnp.exp(jax.random.uniform(key_cols, (1, 1, FF), jnp.float32, 0.0, math.log(10.0)))
    ramp = (3.0 ** (jnp.arange(N_DP, dtype=jnp.float32) / max(N_DP - 1, 1))).reshape(N_DP, 1, 1)
    row_place = (jnp.arange(D, dtype=jnp.float32) / D).reshape(1, D, 1)
    block_width = FF // N_MP
    col_place = ((jnp.arange(FF) % block_width).astype(jnp.float32) / block_width).reshape(1, 1, FF)
    rise = 3.0
    own = jnp.clip(jax.random.normal(key_own, (N_DP, D, FF), jnp.float32), -6.0, 6.0)
    values = ramp * row_scale * col_scale * own
    position = rise ** (row_place - 1.0) * rise ** (col_place - 1.0)
    return (0.01 * values * position).astype(jnp.bfloat16)


def block_scale(stream_key, dims, cuts, smallest, largest):
    gain, own = 1.0, jax.random.fold_in(stream_key, 6)
    for axis_at, parts in cuts:
        draws = jnp.exp(jax.random.uniform(jax.random.fold_in(own, axis_at), (parts,), jnp.float32, smallest / len(cuts), largest / len(cuts)))
        gain = gain * jnp.repeat(draws, dims[axis_at] // parts).reshape([-1 if axis == axis_at else 1 for axis in range(len(dims))])
    return gain


def noise(stream_key, extent, scale, limit, shards=(), held_as=jnp.bfloat16):
    factor_of = block_scale(stream_key, extent, shards, -0.22, 0.18) if shards else 1.0
    drawn = jax.random.normal(stream_key, extent, jnp.float32) * scale * factor_of
    return jnp.minimum(jnp.maximum(drawn, -limit), limit).astype(held_as)


def setup_inputs(seed: int = 0) -> dict:
    arg_keys = jax.random.split(jax.random.key(seed), 5)
    return {
        "tokens": noise(arg_keys[0], (TOKENS, D), 1.0, 6.0, ((0, 8), (1, 4))),
        "ln_gain": jnp.clip(1.0 + 0.1 * jax.random.normal(arg_keys[1], (D,), jnp.float32), 0.5, 1.5).astype(jnp.bfloat16),
        "weights": noise(arg_keys[2], (D, FF), D ** -0.5, 0.078125, ((0, 8), (1, 4))),
        "grad_partials": draw_grad_partials(jax.random.fold_in(arg_keys[4], 71), 0),
    }


def reference(tokens, ln_gain, weights, grad_partials):

    def add_shard(index, total):
        return total + grad_partials[index].astype(jnp.float32)
    grad = lax.fori_loop(0, N_DP, add_shard, jnp.zeros((D, FF), jnp.float32))
    squares = jnp.sum(grad * grad)
    scale = 0.7 * math.sqrt(FF) / jnp.sqrt(squares + 1e-12)
    perturbed = (weights.astype(jnp.float32) + scale * grad).astype(jnp.bfloat16)
    values = tokens.astype(jnp.float32)
    center = lax.optimization_barrier(jnp.mean(values, axis=1, keepdims=True))
    spread = lax.optimization_barrier(jnp.mean((values - center) ** 2, axis=1, keepdims=True))
    normed = ((values - center) / jnp.sqrt(spread + 1e-06) * ln_gain.astype(jnp.float32)).astype(jnp.bfloat16)
    pre = jnp.dot(normed, perturbed, preferred_element_type=jnp.float32)
    hidden = jax.nn.gelu(pre, approximate=False).astype(jnp.bfloat16)
    return (hidden, perturbed)
```

```python
import functools
import math

import jax
import jax.numpy as jnp
from jax import lax
from jax.experimental import pallas as pl
from jax.experimental.pallas import tpu as pltpu
from jax.sharding import PartitionSpec as P

SUBS = 6
AHEAD = 2
VMEM_LIMIT = 66 * 1000 * 1000


def power_of_two(n):
    return n & (n - 1) == 0


def chip_at(pos, n):
    if not power_of_two(n):
        return pos
    bits = n.bit_length() - 1
    out = 0
    for b in range(bits):
        out = out + ((pos // 2**b + pos // 2 ** (b + 1)) % 2) * 2**b
    return out


def position_of(chip, n):
    if not power_of_two(n):
        return chip
    bits = n.bit_length() - 1
    above, out = 0, 0
    for b in reversed(range(bits)):
        above = (chip // 2**b + above) % 2
        out = out + above * 2**b
    return out


def ring(n):
    me = lax.axis_index("dp")
    chip, core = me // 2, me % 2
    pos = position_of(chip, n)
    right = chip_at((pos + 1) % n, n) * 2 + core
    left = chip_at((pos + n - 1) % n, n) * 2 + core
    return pos, core, (right, left), chip * 2 + 1 - core


def greet(peers):
    barrier = pltpu.get_barrier_semaphore()
    for axis, peer in peers:
        pl.semaphore_signal(
            barrier, inc=1, device_id={axis: peer}, device_id_type=pl.DeviceIdType.MESH
        )
    pl.semaphore_wait(barrier, len(peers))


def others(axis, size):
    me = lax.axis_index(axis)
    return [(axis, (me + k) % size) for k in range(1, size)]


def remote(src, dst, send, recv, peer, axis="dp"):
    return pltpu.make_async_remote_copy(
        src_ref=src,
        dst_ref=dst,
        send_sem=send,
        recv_sem=recv,
        device_id={axis: peer},
        device_id_type=pl.DeviceIdType.MESH,
    )


def scatter_kernel(
    n, n_mp, radius, g_ref, w_ref, gain_ref, out_ref, gains_ref,
    part, recv, own, grad, sq_ref, stat, sums, gains,
    part_send, part_recv, hop_send, hop_recv, own_sem,
    stat_send, stat_recv, sums_send, sums_recv, gain_send, gain_recv,
):
    pos, core, hops, partner = ring(n)
    rows, half = part.shape[2], part.shape[3]
    sub = rows // SUBS
    total = n * SUBS
    tile = 16
    dp_peers, mp_peers = others("dp", 2 * n), others("mp", n_mp)
    greet(dp_peers + mp_peers)

    def block(t, d, which):
        s, i = t // SUBS, t % SUBS
        target = (pos + n - 1 - s + n) % n if d == 0 else (pos + 1 + s) % n
        start = (chip_at(target, n) * 2 + which) * rows + i * sub
        return g_ref.at[pl.ds(pl.multiple_of(start, tile), sub), pl.ds(d * half, half)]

    def piece(ref, t, d):
        return ref.at[t // SUBS, d, pl.ds(pl.multiple_of((t % SUBS) * sub, tile), sub)]

    def push(t, d):
        at = t * 2 + d
        return remote(
            block(t, d, 1 - core), piece(part, t, d), part_send.at[at], part_recv.at[at], partner
        )

    def load(t, d):
        return pltpu.make_async_copy(block(t, d, core), own.at[t % 2, d], own_sem.at[(t % 2) * 2 + d])

    def hop(t, d, src):
        at = t * 2 + d
        return remote(piece(src, t, d), piece(recv, t, d), hop_send.at[at], hop_recv.at[at], hops[d])

    for d in range(2):
        load(0, d).start()

    @pl.loop(0, SUBS)
    def _(t):
        for d in range(2):
            push(t, d).start()

    place = lax.axis_index("mp")
    fetch = pltpu.make_async_copy(w_ref, out_ref, own_sem.at[4])
    fetch.start()
    gain_copies = [
        remote(gain_ref, gains.at[place], gain_send.at[k], gain_recv.at[k], peer, axis)
        for k, (axis, peer) in enumerate(mp_peers)
    ]
    for copy in gain_copies:
        copy.start()
    gains[place] = gain_ref[...]
    sq_ref[...] = jnp.zeros_like(sq_ref)

    def step(t, first, last):
        @pl.when(t + 1 < total)
        def _():
            for d in range(2):
                load(t + 1, d).start()

        @pl.when(t + SUBS < total)
        def _():
            for d in range(2):
                push(t + SUBS, d).start()

        for d in range(2):
            load(t, d).wait()
            push(t, d).wait_recv()
            if not first:
                hop(t - SUBS, d, recv).wait_recv()
            source = piece(part, t, d)
            came = None if first else piece(recv, t - SUBS, d)
            mine = own.at[t % 2, d]

            @pl.loop(0, sub // tile)
            def _(r):
                at = pl.ds(pl.multiple_of(r * tile, tile), tile)
                value = mine[at, :].astype(jnp.float32) + source[at, :].astype(jnp.float32)
                if not first:
                    value = value + came[at, :].astype(jnp.float32)
                if last:
                    row = pl.multiple_of((t % SUBS) * sub + r * tile, tile)
                    grad[pl.ds(row, tile), d * half : (d + 1) * half] = value
                    squared = value * value
                    sq_ref[...] += squared[:8] + squared[8:]
                elif first:
                    source[at, :] = value.astype(jnp.bfloat16)
                else:
                    came[at, :] = value.astype(jnp.bfloat16)

        if not last:
            for d in range(2):
                at = t * 2 + d
                src = piece(part, t, d) if first else piece(recv, t - SUBS, d)
                remote(src, piece(recv, t, d), hop_send.at[at], hop_recv.at[at], hops[d]).start()

    @pl.loop(0, SUBS)
    def _(t):
        step(t, True, False)

    @pl.loop(SUBS, total - SUBS)
    def _(t):
        step(t, False, False)

    @pl.loop(total - SUBS, total)
    def _(t):
        step(t, False, True)

    folded = sq_ref[:, :128]
    for c in range(1, half // 128):
        folded = folded + sq_ref[:, c * 128 : (c + 1) * 128]
    stat[0] = folded

    @pl.loop(0, total)
    def _(t):
        for d in range(2):
            push(t, d).wait_send()

    @pl.loop(0, total - SUBS)
    def _(t):
        for d in range(2):
            hop(t, d, recv).wait_send()

    def share(slots, peers, send, arrive):
        copies = [
            remote(slots.at[0], slots.at[k + 1], send.at[k], arrive.at[k], peer, axis)
            for k, (axis, peer) in enumerate(peers)
        ]
        for copy in copies:
            copy.start()
        for copy in copies:
            copy.wait()
        return jnp.sum(slots[...], axis=0)

    sums[0] = share(stat, dp_peers, stat_send, stat_recv)
    for copy in gain_copies:
        copy.wait()
    gains_ref[...] = gains[...]
    fetch.wait()
    every = share(sums, mp_peers, sums_send, sums_recv)
    squares = jnp.sum(jnp.sum(every, axis=0, keepdims=True), axis=1, keepdims=True)
    scale = radius / jnp.sqrt(squares + 1e-12)

    @pl.loop(0, rows // tile)
    def _(r):
        at = pl.ds(pl.multiple_of(r * tile, tile), tile)
        value = out_ref[at, :].astype(jnp.float32) + scale * grad[at, :]
        out_ref[at, :] = value.astype(jnp.bfloat16)


def reduce_rows(n, n_mp, radius, grads, weights, gain):
    depth, cols = grads.shape
    rows, half = depth // (2 * n), cols // 2
    sub = rows // SUBS
    dma = pltpu.SemaphoreType.DMA
    return pl.pallas_call(
        functools.partial(scatter_kernel, n, n_mp, radius),
        out_shape=(
            jax.ShapeDtypeStruct((rows, cols), jnp.bfloat16),
            jax.ShapeDtypeStruct((n_mp, *gain.shape), jnp.float32),
        ),
        in_specs=[
            pl.BlockSpec(memory_space=pl.ANY),
            pl.BlockSpec(memory_space=pl.ANY),
            pl.BlockSpec(memory_space=pltpu.VMEM),
        ],
        out_specs=(
            pl.BlockSpec(memory_space=pltpu.VMEM),
            pl.BlockSpec(memory_space=pltpu.VMEM),
        ),
        scratch_shapes=[
            pltpu.VMEM((n, 2, rows, half), jnp.bfloat16),
            pltpu.VMEM((n - 1, 2, rows, half), jnp.bfloat16),
            pltpu.VMEM((2, 2, sub, half), jnp.bfloat16),
            pltpu.VMEM((rows, cols), jnp.float32),
            pltpu.VMEM((8, half), jnp.float32),
            pltpu.VMEM((2 * n, 8, 128), jnp.float32),
            pltpu.VMEM((n_mp, 8, 128), jnp.float32),
            pltpu.VMEM((n_mp, *gain.shape), jnp.float32),
            dma((n * SUBS * 2,)),
            dma((n * SUBS * 2,)),
            dma(((n - 1) * SUBS * 2,)),
            dma(((n - 1) * SUBS * 2,)),
            dma((5,)),
            dma((2 * n - 1,)),
            dma((2 * n - 1,)),
            dma((n_mp - 1,)),
            dma((n_mp - 1,)),
            dma((n_mp - 1,)),
            dma((n_mp - 1,)),
        ],
        compiler_params=pltpu.CompilerParams(
            collective_id=1, has_side_effects=True, vmem_limit_bytes=VMEM_LIMIT
        ),
        cost_estimate=pl.CostEstimate(
            flops=200 * 10**9, bytes_accessed=3 * grads.size, transcendentals=0
        ),
        name="reduce_rows",
    )(grads, weights, gain)


def gather_kernel(
    n, x_ref, gain_ref, p_ref, out_ref, normed, buf, pre_ref,
    hop_send, hop_recv, part_send, part_recv, own_sem, x_sem,
):
    pos, core, hops, partner = ring(n)
    rows, width = buf.shape[3] // 2, buf.shape[4]
    half = SUBS * width
    greet([("dp", peer) for peer in (*hops, partner)])

    def mine(i, d):
        return p_ref.at[:, pl.ds(pl.multiple_of(d * half + i * width, 128), width)]

    def piece(s, i, d, which):
        return buf.at[s, d, i, pl.ds(pl.multiple_of(which * rows, 16), rows)]

    def hop(s, i, d, src):
        at = ((s - 1) * SUBS + i) * 2 + d
        return remote(src, piece(s, i, d, core), hop_send.at[at], hop_recv.at[at], hops[d])

    def push(s, i, d, src):
        at = (s * SUBS + i) * 2 + d
        return remote(src, piece(s, i, d, core), part_send.at[at], part_recv.at[at], partner)

    def pushed(s, i, d):
        at = (s * SUBS + i) * 2 + d
        there = piece(s, i, d, 1 - core)
        return remote(there, there, part_send.at[at], part_recv.at[at], partner)

    def keep(i, d):
        return pltpu.make_async_copy(mine(i, d), piece(0, i, d, core), own_sem.at[i * 2 + d])

    fetch = pltpu.make_async_copy(x_ref, normed, x_sem.at[0])
    fetch.start()
    for i in range(AHEAD):
        for d in range(2):
            hop(1, i, d, mine(i, d)).start()

    @pl.loop(0, SUBS)
    def _(i):
        for d in range(2):
            keep(i, d).start()
            push(0, i, d, mine(i, d)).start()

    pre_ref[...] = jnp.zeros_like(pre_ref)
    fetch.wait()

    @pl.loop(0, normed.shape[0] // 16)
    def _(r):
        at = pl.ds(pl.multiple_of(r * 16, 16), 16)
        values = normed[at, :].astype(jnp.float32)
        center = jnp.mean(values, axis=1, keepdims=True)
        moved = values - center
        spread = jnp.mean(moved * moved, axis=1, keepdims=True)
        scaled = moved * (1.0 / jnp.sqrt(spread + 1e-06)) * gain_ref[...]
        normed[at, :] = scaled.astype(jnp.bfloat16)

    def multiply(s, i):
        for d in range(2):
            pushed(s, i, d).wait_recv()
            owner = (pos + n - s) % n if d == 0 else (pos + s) % n
            cols = pl.ds(pl.multiple_of(chip_at(owner, n) * 2 * rows, 128), 2 * rows)
            out = pl.ds(pl.multiple_of(d * half + i * width, 128), width)
            pre_ref[:, out] += jnp.dot(
                normed[:, cols], buf[s, d, i], preferred_element_type=jnp.float32
            )

    def activate(i):
        tall = 64
        for d in range(2):
            cols = pl.ds(pl.multiple_of(d * half + i * width, 128), width)

            @pl.loop(0, pre_ref.shape[0] // tall)
            def _(r):
                at = pl.ds(pl.multiple_of(r * tall, tall), tall)
                pre = pre_ref[at, cols]
                value = 0.5 * pre * (1.0 + lax.erf(pre * math.sqrt(0.5)))
                out_ref[at, cols] = value.astype(jnp.bfloat16)

    @pl.loop(0, SUBS + n - 1)
    def _(wave):
        @pl.when(wave + AHEAD < SUBS)
        def _():
            for d in range(2):
                hop(1, wave + AHEAD, d, mine(wave + AHEAD, d)).start()

        for s in range(1, n):
            i = wave - (s - 1)

            @pl.when((i >= 0) & (i < SUBS))
            def _():
                for d in range(2):
                    hop(s, i, d, piece(s, i, d, core)).wait_recv()
                    if s < n - 1:
                        hop(s + 1, i, d, piece(s, i, d, core)).start()
                    push(s, i, d, piece(s, i, d, core)).start()

            if s == 1:

                @pl.when(wave < SUBS)
                def _():
                    for d in range(2):
                        keep(wave, d).wait()
                    multiply(0, wave)

            @pl.when((i >= 1) & (i <= SUBS))
            def _():
                multiply(s, i - 1)
                if s == n - 1:
                    activate(i - 1)

    @pl.loop(0, SUBS)
    def _(i):
        for d in range(2):
            for s in range(n):
                push(s, i, d, piece(s, i, d, core)).wait_send()
            for s in range(1, n):
                hop(s, i, d, piece(s, i, d, core)).wait_send()


def gather_matmul(n, feats, gains, perturbed):
    tokens, depth = feats.shape
    rows, cols = perturbed.shape
    half = cols // 2
    dma = pltpu.SemaphoreType.DMA
    return pl.pallas_call(
        functools.partial(gather_kernel, n),
        out_shape=jax.ShapeDtypeStruct((tokens, cols), jnp.bfloat16),
        in_specs=[
            pl.BlockSpec(memory_space=pl.ANY),
            pl.BlockSpec(memory_space=pltpu.VMEM),
            pl.BlockSpec(memory_space=pl.ANY),
        ],
        out_specs=pl.BlockSpec(memory_space=pltpu.VMEM),
        scratch_shapes=[
            pltpu.VMEM((tokens, depth), jnp.bfloat16),
            pltpu.VMEM((n, 2, SUBS, 2 * rows, half // SUBS), jnp.bfloat16),
            pltpu.VMEM((tokens, cols), jnp.float32),
            dma(((n - 1) * SUBS * 2,)),
            dma(((n - 1) * SUBS * 2,)),
            dma((n * SUBS * 2,)),
            dma((n * SUBS * 2,)),
            dma((SUBS * 2,)),
            dma((1,)),
        ],
        compiler_params=pltpu.CompilerParams(
            collective_id=2, has_side_effects=True, vmem_limit_bytes=VMEM_LIMIT
        ),
        cost_estimate=pl.CostEstimate(
            flops=2 * tokens * depth * cols,
            bytes_accessed=2 * depth * cols,
            transcendentals=0,
        ),
        name="gather_matmul",
    )(feats, gains, perturbed)


def per_device(n, n_mp, width, tokens, ln_gain, weights, grad_partials):
    feats = lax.all_gather(tokens, "mp", axis=1, tiled=True)
    gain = jnp.broadcast_to(ln_gain.astype(jnp.float32), (8, ln_gain.shape[0]))
    radius = 0.7 * math.sqrt(width)
    perturbed, gains = reduce_rows(n, n_mp, radius, grad_partials[0], weights, gain)
    hidden = gather_matmul(n, feats, gains[:, 0].reshape(1, -1), perturbed)
    return (hidden, perturbed)


def solution(mesh):
    placed = (P("dp", "mp"), P("mp"), P("dp", "mp"), P("dp", None, "mp"))

    def whole(tokens, ln_gain, weights, grad_partials):
        return jax.shard_map(
            functools.partial(per_device, mesh.shape["dp"] // 2, mesh.shape["mp"], weights.shape[1]),
            mesh=mesh,
            in_specs=placed,
            out_specs=(P("dp", "mp"), P("dp", "mp")),
            check_vma=False,
        )(tokens, ln_gain, weights, grad_partials)

    return whole
```
